32 devices in a mesh: seq: 8 (over z, x), head: 4 (over y, core).
Axes of the slice: x: 2, y: 2, z: 4, core: 2. Of those that a mesh axis runs over, the one named last changes fastest.
Arguments:
- query_in: bfloat16 [2048, 8192], P('seq', 'head'), may hold values from -1.796875 to 1.796875
- key_in: bfloat16 [2048, 8192], P('seq', 'head'), may hold values from -1.796875 to 1.796875
- value_in: bfloat16 [2048, 8192], P('seq', 'head'), may hold values from -11 to 11
- log_decay: float32 [2048, 64], P('seq', 'head'), may hold values from -1 to 0, as said below
- norm_gain: float32 [8192], P('head'), may hold values from 0.5 to 1.5
- prompt_lengths: int32 [4], replicated, may hold values from 1 to 1536, 2048 in all
- step_query: bfloat16 [4, 128, 8192], P(None, 'seq', 'head'), may hold values from -1.796875 to 1.796875
- step_key: bfloat16 [4, 128, 8192], P(None, 'seq', 'head'), may hold values from -1.796875 to 1.796875
- step_value: bfloat16 [4, 128, 8192], P(None, 'seq', 'head'), may hold values from -6 to 6
- step_decay: float32 [4, 128, 64], P(None, 'seq', 'head'), may hold values from -0.3 to -0.01
- row_prompt: int32 [128], P('seq'), may hold values from 0 to 3
Outputs:
- attn_out: bfloat16 [2048, 8192], P('seq', 'head')
- decode_out: bfloat16 [4, 128, 8192], P(None, 'seq', 'head')
The draws below stay inside these ranges and needn't reach their ends.
Inputs may be any that keep to these rules, and one draw needn't show every extreme that they name: `log_decay`: Negative; per head and token.
All inputs are finite; a program needn't handle non-finite values.
Results may differ from the reference program's by a relative error of at most 0.0056.
Values sent between devices are 32-bit elements; how exact they have to be, the bound alone decides.
A program may use at most 64 MiB of HBM per device.

```python
import math
import jax
import jax.numpy as jnp
import numpy as np
from jax import lax

HEAD_COUNT = 64
HDIM = 128
TOK_DEV = 256
BLOCK = 256
PROMPTS = 4
STEPS = 4
PROMPT_TOKENS = 2048
ROWS = 128


def draw_log_decay(key, part):
    fragments = jax.random.split(jax.random.fold_in(key, 11), 7)
    order = jax.random.permutation(fragments[0], HEAD_COUNT)
    fast = order < HEAD_COUNT // 2
    slow_rate = jnp.exp(jax.random.uniform(fragments[1], (HEAD_COUNT,), jnp.float32, jnp.log(0.2), jnp.log(1.0))) / PROMPT_TOKENS
    fast_rate = jnp.exp(jax.random.uniform(fragments[2], (HEAD_COUNT,), jnp.float32, jnp.log(1.0 / 50.0), jnp.log(1.0 / 30.0)))
    decay_rate = jnp.where(fast, fast_rate, slow_rate)
    spans = PROMPT_TOKENS // TOK_DEV
    device_multiplier = jnp.exp(jax.random.uniform(fragments[3], (spans, HEAD_COUNT), jnp.float32, -0.7, 0.7))
    device_multiplier = jnp.repeat(device_multiplier, TOK_DEV, axis=0)
    coarse_estimate = jax.random.uniform(fragments[4], (PROMPT_TOKENS, HEAD_COUNT), jnp.float32, 0.5, 1.5)
    spike_positions = jax.random.randint(fragments[5], (4,), 0, PROMPT_TOKENS)
    marked_rows = jnp.any(jnp.arange(PROMPT_TOKENS)[:, None] == spike_positions[None, :], axis=1)
    spike_group = jnp.log(jax.random.uniform(fragments[6], (PROMPT_TOKENS, HEAD_COUNT), jnp.float32, 0.5, 0.8))
    return (-decay_rate[None, :] * device_multiplier * coarse_estimate + jnp.where(marked_rows[:, None], spike_group, 0.0)).astype(jnp.float32)


def draw_value_in(key, part):
    fragments = jax.random.split(jax.random.fold_in(key, 23), 1)
    head_of = (jnp.arange(HEAD_COUNT * HDIM) // HDIM).astype(jnp.float32)
    scale = 0.5 * 3.0 ** (head_of / max(HEAD_COUNT - 1, 1))
    base = jnp.clip(jax.random.normal(fragments[0], (PROMPT_TOKENS, HEAD_COUNT * HDIM), jnp.float32), -4.0, 4.0)
    return (base * scale[None, :]).astype(jnp.bfloat16)


def place_ends(result, own_key, least, top_value):
    longest = result.shape.index(max(result.shape))
    spots = []
    for shift in (0, 1):
        where = [jax.random.randint(jax.random.fold_in(own_key, axis), (), 0, length) for axis, length in enumerate(result.shape)]
        where[longest] = (where[longest] + shift) % result.shape[longest]
        spots.append(tuple(where))
    return result.at[spots[0]].set(least).at[spots[1]].set(top_value)


def shard_levels(stream_key, dims, pieces, low, top_value):
    level = 1.0
    for position, parts in pieces:
        heights = jax.random.uniform(jax.random.fold_in(jax.random.fold_in(stream_key, 6), position), (parts,), jnp.float32, low / len(pieces), top_value / len(pieces))
        level = level * jnp.repeat(jnp.exp(heights), dims[position] // parts).reshape((-1,) + (1,) * (len(dims) - 1 - position))
    return level


def split_up(count, total, limit, lean):
    portions = [(1 << 20) // math.isqrt(grade ** lean) + 1 for grade in range(2, count + 1)]
    spare, counts = total - limit - (count - 1), [1] * (count - 1)
    while spare > 0:
        candidates = [i for i in range(count - 1) if counts[i] < limit]
        mass, remaining = sum([portions[i] for i in candidates]), spare
        for i in candidates:
            more = min(limit - counts[i], max(1, remaining * portions[i] // mass), spare)
            counts[i] = counts[i] + more
            spare = spare - more
    return np.array([limit] + counts)


def ragged_sizes(own_key, count, total, bound, lean):
    if count == 2:
        one = jax.random.randint(own_key, (), max(1, total - bound), min(bound, total - 1) + 1)
        return jnp.stack([one, total - one])
    sizes = jnp.asarray(split_up(count, total, bound, lean), jnp.int32)
    pairs = (count - 1) // 2
    giver, sink = sizes[1:1 + 2 * pairs:2], sizes[2:2 + 2 * pairs:2]
    margin = jnp.minimum(giver - 1, bound - sink)
    moved = jax.random.randint(jax.random.fold_in(own_key, 1), (pairs,), 0, 1 << 20) % (margin + 1)
    sizes = sizes.at[1:1 + 2 * pairs:2].set(giver - moved).at[2:2 + 2 * pairs:2].set(sink + moved)
    return sizes[jax.random.permutation(jax.random.fold_in(own_key, 2), count)]


def gaussian(rng, dims, scale, most, pieces=(), kind=jnp.bfloat16):
    values = scale * jax.random.normal(rng, dims, jnp.float32)
    if pieces:
        values = values * shard_levels(rng, dims, pieces, -0.22, 0.18)
    return jnp.clip(values, -most, most).astype(kind)


def setup_inputs(seed: int = 0) -> dict:
    streams_of = jax.random.split(jax.random.key(seed), 12)
    return {
        "query_in": gaussian(streams_of[0], (PROMPT_TOKENS, HEAD_COUNT * HDIM), 0.3, 1.796875, ((0, 8), (1, 4))),
        "key_in": gaussian(streams_of[1], (PROMPT_TOKENS, HEAD_COUNT * HDIM), 0.3, 1.796875, ((0, 8), (1, 4))),
        "value_in": draw_value_in(jax.random.fold_in(streams_of[11], 71), 0),
        "log_decay": draw_log_decay(jax.random.fold_in(streams_of[11], 71), 0),
        "norm_gain": jnp.clip(1.0 + 0.1 * jax.random.normal(streams_of[4], (HEAD_COUNT * HDIM,), jnp.float32), 0.5, 1.5),
        "prompt_lengths": ragged_sizes(streams_of[5], PROMPTS, PROMPT_TOKENS, PROMPT_TOKENS * 3 // 4, 2).astype(jnp.int32),
        "step_query": gaussian(streams_of[6], (STEPS, ROWS, HEAD_COUNT * HDIM), 0.3, 1.796875, ((1, 8), (2, 4))),
        "step_key": gaussian(streams_of[7], (STEPS, ROWS, HEAD_COUNT * HDIM), 0.3, 1.796875, ((1, 8), (2, 4))),
        "step_value": gaussian(streams_of[8], (STEPS, ROWS, HEAD_COUNT * HDIM), 1.0, 6.0, ((1, 8), (2, 4))),
        "step_decay": jnp.clip(-0.3 + 0.29000001 * jax.random.uniform(streams_of[9], (STEPS, ROWS, HEAD_COUNT), jnp.float32) ** shard_levels(streams_of[9], (STEPS, ROWS, HEAD_COUNT), ((1, 8), (2, 4)), -0.2, 0.2), -0.3, -0.01),
        "row_prompt": place_ends(jax.random.randint(streams_of[10], (ROWS,), 0, PROMPTS), jax.random.fold_in(streams_of[10], 1), 0, PROMPTS - 1).astype(jnp.int32),
    }


EPSILON = 1e-06

def segment_ids(prompt_lengths, positions):
    boundary = jnp.cumsum(prompt_lengths).astype(jnp.int32)
    return lax.optimization_barrier(jnp.sum((positions[:, None] >= boundary[None, :]).astype(jnp.int32), axis=1)).astype(jnp.int32)

def half_round(array):
    return lax.optimization_barrier(array.astype(jnp.bfloat16)).astype(jnp.float32)

def block_pass(query_blk, key_blk, value_blk, decay_blk, seg_blk, seg_front, state):
    cumul = jnp.cumsum(decay_blk, axis=0)
    length = seg_blk.shape[0]
    causal = jnp.arange(length)[:, None] >= jnp.arange(length)[None, :]
    linked = causal & (seg_blk[:, None] == seg_blk[None, :])
    spread = cumul[:, None, :] - cumul[None, :, :]
    factor = jnp.where(linked[:, :, None], jnp.exp(jnp.where(linked[:, :, None], spread, 0.0)), 0.0)
    query_f = query_blk.astype(jnp.float32)
    key_f = key_blk.astype(jnp.float32)
    value_f = value_blk.astype(jnp.float32)
    scores = jnp.einsum('thd,shd->hts', query_f, key_f)
    weights = half_round(scores * jnp.transpose(factor, (2, 0, 1)))
    inner = jnp.einsum('hts,shd->thd', weights, value_f)
    carried = jnp.exp(cumul) * (seg_blk == seg_front).astype(jnp.float32)[:, None]
    state_half = half_round(state)
    outer = jnp.einsum('thd,hde->the', query_f, state_half) * carried[:, :, None]
    keep = jnp.exp(cumul[-1:] - cumul) * (seg_blk == seg_blk[-1]).astype(jnp.float32)[:, None]
    keyed = half_round(key_f * keep[:, :, None])
    update = jnp.einsum('shd,she->hde', keyed, value_f)
    onward = jnp.exp(cumul[-1]) * (seg_blk[-1] == seg_front).astype(jnp.float32)
    new_state = onward[:, None, None] * state + update
    return (inner + outer, new_state)

def reference(query_in, key_in, value_in, log_decay, norm_gain, prompt_lengths, step_query, step_key, step_value, step_decay, row_prompt):
    nblocks = PROMPT_TOKENS // BLOCK
    positions = jnp.arange(PROMPT_TOKENS, dtype=jnp.int32)
    segs = segment_ids(prompt_lengths, positions)
    seg_prior = jnp.concatenate([jnp.full((1,), -1, jnp.int32), segs[:-1]]).astype(jnp.int32)
    shape4 = (nblocks, BLOCK, HEAD_COUNT, HDIM)
    inputs = (query_in.reshape(shape4), key_in.reshape(shape4), value_in.reshape(shape4), log_decay.reshape(nblocks, BLOCK, HEAD_COUNT), segs.reshape(nblocks, BLOCK), seg_prior.reshape(nblocks, BLOCK)[:, 0])

    def stepper(state, fragments):
        mixed_blk, new_state = block_pass(fragments[0], fragments[1], fragments[2], fragments[3], fragments[4], fragments[5], state)
        return (new_state, (mixed_blk, state))
    initial = jnp.zeros((HEAD_COUNT, HDIM, HDIM), jnp.float32)
    final_state, (mixed_all, starts) = lax.scan(stepper, initial, inputs)
    mixed = mixed_all.reshape(PROMPT_TOKENS, HEAD_COUNT * HDIM)
    scale = lax.rsqrt(lax.optimization_barrier(jnp.sum(mixed * mixed, axis=1)) / (HEAD_COUNT * HDIM) + EPSILON)
    attn_out = (mixed * scale[:, None] * norm_gain[None, :]).astype(jnp.bfloat16)
    boundary = jnp.cumsum(prompt_lengths).astype(jnp.int32)

    def prompt_end(prompt):
        last_tok = (boundary[prompt] - 1).astype(jnp.int32)
        blk_index = (last_tok // BLOCK).astype(jnp.int32)
        offset = (last_tok - blk_index * BLOCK).astype(jnp.int32)
        begin = (blk_index * BLOCK).astype(jnp.int32)
        key_blk = lax.dynamic_slice_in_dim(key_in, begin, BLOCK, 0).reshape(BLOCK, HEAD_COUNT, HDIM).astype(jnp.float32)
        value_blk = lax.dynamic_slice_in_dim(value_in, begin, BLOCK, 0).reshape(BLOCK, HEAD_COUNT, HDIM).astype(jnp.float32)
        decay_blk = lax.dynamic_slice_in_dim(log_decay, begin, BLOCK, 0)
        seg_blk = lax.dynamic_slice_in_dim(segs, begin, BLOCK, 0)
        seg_front = seg_prior[begin]
        cumul = jnp.cumsum(decay_blk, axis=0)
        reached = cumul[offset]
        taken = (jnp.arange(BLOCK) <= offset) & (seg_blk == prompt)
        keep_end = jnp.exp(jnp.where(taken[:, None], reached[None, :] - cumul, 0.0)) * taken.astype(jnp.float32)[:, None]
        tailed = half_round(key_blk * keep_end[:, :, None])
        part = jnp.einsum('shd,she->hde', tailed, value_blk)
        lead = jnp.exp(reached) * (seg_front == prompt).astype(jnp.float32)
        return lead[:, None, None] * starts[blk_index] + part
    prompt_state = lax.map(prompt_end, jnp.arange(PROMPTS, dtype=jnp.int32))

    def decode_row(fragments):
        prompt, queries, keyset, valueset, decays = fragments
        row_state = prompt_state[prompt]
        results = []
        for section in range(STEPS):
            query_now = queries[section].astype(jnp.float32).reshape(HEAD_COUNT, HDIM)
            key_now = keyset[section].astype(jnp.float32).reshape(HEAD_COUNT, HDIM)
            value_now = valueset[section].astype(jnp.float32).reshape(HEAD_COUNT, HDIM)
            row_state = jnp.exp(decays[section])[:, None, None] * row_state + key_now[:, :, None] * value_now[:, None, :]
            results.append(jnp.einsum('hd,hde->he', query_now, row_state, precision=lax.Precision.HIGHEST).reshape(HEAD_COUNT * HDIM))
        return jnp.stack(results)
    decoded = lax.map(decode_row, (row_prompt, jnp.transpose(step_query, (1, 0, 2)), jnp.transpose(step_key, (1, 0, 2)), jnp.transpose(step_value, (1, 0, 2)), jnp.transpose(step_decay, (1, 0, 2))))
    decoded = jnp.transpose(decoded, (1, 0, 2))
    step_scale = lax.rsqrt(lax.optimization_barrier(jnp.sum(decoded * decoded, axis=2)) / (HEAD_COUNT * HDIM) + EPSILON)
    decode_out = (decoded * step_scale[:, :, None] * norm_gain[None, None, :]).astype(jnp.bfloat16)
    return (attn_out, decode_out)
```

```python
import functools

import jax
import jax.numpy as jnp
from jax import lax
from jax.experimental import pallas as pl
from jax.experimental.pallas import tpu as pltpu
from jax.sharding import PartitionSpec as P

HEAD_COUNT = 64
HDIM = 128
BLOCK = 256
PROMPTS = 4
PAIR = 2


EPSILON = 1e-06
MESH = pl.DeviceIdType.MESH


def exchange_kernel(
    n,
    part_ref,
    coef_ref,
    mask_ref,
    query_ref,
    row_ref,
    entry_ref,
    dec_ref,
    x_recv,
    coef_recv,
    q_recv,
    row_recv,
    f_recv,
    f_send,
    b_recv,
    b_send,
    e_send,
    e_recv,
    r_send,
    r_recv,
    xs_sem,
    xr_sem,
    cs_sem,
    cr_sem,
    qs_sem,
    qr_sem,
    ws_sem,
    wr_sem,
    fs_sem,
    fr_sem,
    bs_sem,
    br_sem,
    es_sem,
    er_sem,
    rs_sem,
    rr_sem,
):
    me = lax.axis_index("seq")
    side = lax.rem(me, PAIR)
    rank = me // PAIR
    ranks = n // PAIR
    partner = me + 1 - 2 * side
    heads = part_ref.shape[0]
    half = heads // PAIR
    slots = part_ref.shape[1]
    mine = side * half
    theirs = (1 - side) * half
    is_first = rank == 0
    is_last = rank == ranks - 1
    ahead = lax.rem(me + PAIR, n)
    behind = lax.rem(me + n - PAIR, n)

    def copy(src, dst, send, recv, to):
        return pltpu.make_async_remote_copy(
            src_ref=src,
            dst_ref=dst,
            send_sem=send,
            recv_sem=recv,
            device_id={"seq": to},
            device_id_type=MESH,
        )

    def x_copy(j, p):
        i = j * slots + p
        return copy(part_ref.at[theirs + j, p], x_recv.at[j, p], xs_sem.at[i], xr_sem.at[i], partner)

    def f_copy(j, p):
        i = j * slots + p
        return copy(f_send.at[j, p], f_recv.at[j, p], fs_sem.at[i], fr_sem.at[i], ahead)

    def b_copy(j, p):
        i = j * slots + p
        return copy(b_send.at[j, p], b_recv.at[j, p], bs_sem.at[i], br_sem.at[i], behind)

    def e_copy(j):
        return copy(e_send.at[j], e_recv.at[j], es_sem.at[j], er_sem.at[j], partner)

    def r_copy(j):
        return copy(r_send.at[j], r_recv.at[j], rs_sem.at[j], rr_sem.at[j], partner)

    coef_copy = copy(coef_ref.at[pl.ds(theirs, half)], coef_recv, cs_sem, cr_sem, partner)
    row_copy = copy(row_ref, row_recv, ws_sem, wr_sem, partner)
    q_copy = copy(query_ref.at[pl.ds(theirs, half)], q_recv, qs_sem, qr_sem, partner)

    barrier = pltpu.get_barrier_semaphore()
    pl.semaphore_signal(barrier, inc=1, device_id={"seq": partner}, device_id_type=MESH)

    @pl.when(jnp.logical_not(is_last))
    def _():
        pl.semaphore_signal(barrier, inc=1, device_id={"seq": ahead}, device_id_type=MESH)

    @pl.when(jnp.logical_not(is_first))
    def _():
        pl.semaphore_signal(barrier, inc=1, device_id={"seq": behind}, device_id_type=MESH)

    pl.semaphore_wait(barrier, 1 + jnp.where(is_first, 0, 1) + jnp.where(is_last, 0, 1))

    coef_copy.start()

    @pl.loop(0, half)
    def _(j):
        for p in range(slots):
            x_copy(j, p).start()

    row_copy.start()
    q_copy.start()

    @pl.when(is_first)
    def _():
        f_recv[...] = jnp.zeros_like(f_recv)

    @pl.when(is_last)
    def _():
        b_recv[...] = jnp.zeros_like(b_recv)

    coef_copy.wait()

    lag = jnp.where(is_last, 0, ranks - rank)
    low = side == 0

    def forward(j):
        acc_mine = None
        acc_theirs = None
        for p in range(slots):
            x_copy(j, p).wait_recv()

            @pl.when(jnp.logical_not(is_first))
            def _():
                f_copy(j, p).wait_recv()

            own = part_ref[mine + j, p]
            other = x_recv[j, p]
            c_own = coef_ref[mine + j, pl.ds(p, 1), :]
            c_other = coef_recv[j, pl.ds(p, 1), :]
            came = f_recv[j, p]
            middle = jnp.where(low, c_own, c_other) * came + jnp.where(low, own, other)
            after = jnp.where(low, c_other, c_own) * middle + jnp.where(low, other, own)
            f_send[j, p] = after

            @pl.when(jnp.logical_not(is_last))
            def _():
                f_copy(j, p).start()

            at_low = came * mask_ref[pl.ds(p, 1), :]
            at_high = middle * mask_ref[pl.ds(slots + p, 1), :]
            to_mine = jnp.where(low, at_low, at_high)
            to_theirs = jnp.where(low, at_high, at_low)
            acc_mine = to_mine if p == 0 else acc_mine + to_mine
            acc_theirs = to_theirs if p == 0 else acc_theirs + to_theirs
        entry_ref[mine + j] = acc_mine
        e_send[j] = acc_theirs
        e_copy(j).start()

    def backward(j):
        q_own = query_ref[mine + j].astype(jnp.bfloat16)
        q_other = q_recv[j].astype(jnp.bfloat16)
        total_own = None
        total_other = None
        for p in range(slots):

            @pl.when(jnp.logical_not(is_last))
            def _():
                b_copy(j, p).wait_recv()

            ended = mask_ref[pl.ds(2 * slots + p, 1), :]
            final = ended * f_send[j, p] + (1.0 - ended) * b_recv[j, p]
            b_send[j, p] = final

            @pl.when(jnp.logical_not(is_first))
            def _():
                b_copy(j, p).start()

            final_half = final.astype(jnp.bfloat16)
            got_own = jnp.dot(q_own, final_half, preferred_element_type=jnp.float32)
            got_other = jnp.dot(q_other, final_half, preferred_element_type=jnp.float32)
            got_own = jnp.where(row_ref[...] == float(p), got_own, 0.0)
            got_other = jnp.where(row_recv[...] == float(p), got_other, 0.0)
            total_own = got_own if p == 0 else total_own + got_own
            total_other = got_other if p == 0 else total_other + got_other
        dec_ref[mine + j] = total_own
        r_send[j] = total_other
        r_copy(j).start()

    row_copy.wait()
    q_copy.wait()

    @pl.loop(0, half + ranks)
    def _(t):
        @pl.when(t < half)
        def _():
            forward(t)

        @pl.when((t >= lag) & (t < half + lag))
        def _():
            backward(t - lag)

    @pl.loop(0, half)
    def _(j):
        e_copy(j).wait()
        entry_ref[theirs + j] = e_recv[j]
        r_copy(j).wait()
        dec_ref[theirs + j] = r_recv[j]
        for p in range(slots):
            x_copy(j, p).wait_send()

            @pl.when(jnp.logical_not(is_last))
            def _():
                f_copy(j, p).wait_send()

            @pl.when(jnp.logical_not(is_first))
            def _():
                b_copy(j, p).wait_send()


def exchange(n, parts, coef, masks, queries, rows):
    heads, slots = parts.shape[:2]
    half = heads // PAIR
    vectors = queries.shape[1]
    chunks = half * slots
    f32 = jnp.float32
    vmem = pl.BlockSpec(memory_space=pltpu.VMEM)
    dma = pltpu.SemaphoreType.DMA
    states = (half, slots, HDIM, HDIM)
    return pl.pallas_call(
        functools.partial(exchange_kernel, n),
        out_shape=(
            jax.ShapeDtypeStruct((heads, HDIM, HDIM), f32),
            jax.ShapeDtypeStruct((heads, vectors, HDIM), f32),
        ),
        in_specs=[vmem] * 5,
        out_specs=(vmem, vmem),
        scratch_shapes=[
            pltpu.VMEM(states, f32),
            pltpu.VMEM((half,) + coef.shape[1:], f32),
            pltpu.VMEM((half, vectors, HDIM), f32),
            pltpu.VMEM((vectors, HDIM), f32),
            pltpu.VMEM(states, f32),
            pltpu.VMEM(states, f32),
            pltpu.VMEM(states, f32),
            pltpu.VMEM(states, f32),
            pltpu.VMEM((half, HDIM, HDIM), f32),
            pltpu.VMEM((half, HDIM, HDIM), f32),
            pltpu.VMEM((half, vectors, HDIM), f32),
            pltpu.VMEM((half, vectors, HDIM), f32),
            dma((chunks,)),
            dma((chunks,)),
            dma,
            dma,
            dma,
            dma,
            dma,
            dma,
            dma((chunks,)),
            dma((chunks,)),
            dma((chunks,)),
            dma((chunks,)),
            dma((half,)),
            dma((half,)),
            dma((half,)),
            dma((half,)),
        ],
        compiler_params=pltpu.CompilerParams(
            collective_id=0, has_side_effects=True, vmem_limit_bytes=48 * 1024 * 1024
        ),
        name="exchange",
    )(parts, coef, masks, queries, rows)


def segment_ids(prompt_lengths, positions):
    boundary = jnp.cumsum(prompt_lengths)
    return jnp.sum((positions[:, None] >= boundary[None, :]).astype(jnp.int32), axis=1)


def local(
    n,
    query_in,
    key_in,
    value_in,
    log_decay,
    norm_gain,
    prompt_lengths,
    step_query,
    step_key,
    step_value,
    step_decay,
    row_prompt,
):
    f32 = jnp.float32
    tok = query_in.shape[0]
    heads = log_decay.shape[1]
    steps, rows = step_query.shape[:2]
    place = lax.axis_index("seq")
    first = place * tok
    pair_first = (place // PAIR) * (PAIR * tok)
    ends = jnp.cumsum(prompt_lengths)
    begins = ends - prompt_lengths
    segs = segment_ids(prompt_lengths, first + jnp.arange(tok, dtype=jnp.int32))
    slot = jnp.arange(PROMPTS, dtype=jnp.int32)

    def seg_before(token):
        return jnp.where(token > 0, segment_ids(prompt_lengths, (token - 1)[None])[0], -1)

    seg_front = seg_before(first)
    queries = query_in.reshape(tok, heads, HDIM)
    keys = key_in.reshape(tok, heads, HDIM)
    values = value_in.reshape(tok, heads, HDIM)
    cum = jnp.cumsum(log_decay, axis=0)

    last = jnp.clip(ends - first, 1, tok) - 1
    reached = jnp.sum(
        jnp.where((jnp.arange(tok)[None, :] == last[:, None])[:, :, None], cum[None], 0.0), axis=1
    )
    taken = (segs[None, :] == slot[:, None])[:, :, None]
    keep = jnp.where(taken, jnp.exp(jnp.where(taken, reached[:, None, :] - cum[None], 0.0)), 0.0)
    keyed = (keys.astype(f32)[None] * keep[..., None]).astype(jnp.bfloat16)
    parts = jnp.einsum("pshd,she->hpde", keyed, values, preferred_element_type=f32)
    coef = jnp.where(
        (ends <= first)[:, None], 1.0, jnp.where((begins < first)[:, None], jnp.exp(reached), 0.0)
    )
    coef = jnp.broadcast_to(coef.T[:, :, None], (heads, PROMPTS, HDIM))
    pair_last = pair_first + PAIR * tok
    marks = jnp.concatenate(
        [slot == seg_before(pair_first), slot == seg_before(pair_first + tok), ends <= pair_last]
    )
    marks = jnp.concatenate([marks, jnp.zeros((4,), bool)])
    masks = jnp.broadcast_to(marks.astype(f32)[:, None], (marks.shape[0], HDIM))

    step_q = step_query.reshape(steps, rows, heads, HDIM)
    vectors = jnp.transpose(step_q, (2, 0, 1, 3)).reshape(heads, steps * rows, HDIM).astype(f32)
    row_marks = jnp.broadcast_to(
        jnp.broadcast_to(row_prompt.astype(f32)[None, :], (steps, rows)).reshape(-1, 1),
        (steps * rows, HDIM),
    )
    entry, from_state = exchange(n, parts, coef, masks, vectors, row_marks)

    causal = jnp.arange(tok)[:, None] >= jnp.arange(tok)[None, :]
    linked = (causal & (segs[:, None] == segs[None, :]))[None]
    cum_heads = cum.T
    spread = cum_heads[:, :, None] - cum_heads[:, None, :]
    factor = jnp.where(linked, jnp.exp(jnp.where(linked, spread, 0.0)), 0.0)
    scores = jnp.einsum("thd,shd->hts", queries, keys, preferred_element_type=f32)
    weights = (scores * factor).astype(jnp.bfloat16)
    inner = jnp.einsum("hts,shd->thd", weights, values, preferred_element_type=f32)
    carried = jnp.exp(cum) * (segs == seg_front).astype(f32)[:, None]
    outer = (
        jnp.einsum("thd,hde->the", queries, entry.astype(jnp.bfloat16), preferred_element_type=f32)
        * carried[..., None]
    )
    mixed = (inner + outer).reshape(tok, heads * HDIM)

    step_k = step_key.reshape(steps, rows, heads, HDIM).astype(f32)
    step_v = step_value.reshape(steps, rows, heads, HDIM).astype(f32)
    step_qf = step_q.astype(f32)
    from_state = jnp.transpose(from_state.reshape(heads, steps, rows, HDIM), (1, 2, 0, 3))
    results = []
    for i in range(steps):
        decay = step_decay[i]
        total = jnp.sum(step_qf[i] * step_k[i], axis=-1)[..., None] * step_v[i]
        for j in range(i - 1, -1, -1):
            weight = jnp.exp(decay) * jnp.sum(step_qf[i] * step_k[j], axis=-1)
            total = total + weight[..., None] * step_v[j]
            decay = decay + step_decay[j]
        results.append(total + jnp.exp(decay)[..., None] * from_state[i])
    decoded = jnp.stack(results).reshape(steps, rows, heads * HDIM)

    squares, step_squares = lax.psum(
        (jnp.sum(mixed * mixed, axis=1), jnp.sum(decoded * decoded, axis=2)), "head"
    )
    scale = lax.rsqrt(squares / (HEAD_COUNT * HDIM) + EPSILON)
    attn_out = (mixed * scale[:, None] * norm_gain[None, :]).astype(jnp.bfloat16)
    step_scale = lax.rsqrt(step_squares / (HEAD_COUNT * HDIM) + EPSILON)
    decode_out = (decoded * step_scale[:, :, None] * norm_gain[None, None, :]).astype(jnp.bfloat16)
    return (attn_out, decode_out)


def solution(mesh):
    in_specs = (
        P("seq", "head"),
        P("seq", "head"),
        P("seq", "head"),
        P("seq", "head"),
        P("head"),
        P(),
        P(None, "seq", "head"),
        P(None, "seq", "head"),
        P(None, "seq", "head"),
        P(None, "seq", "head"),
        P("seq"),
    )
    out_specs = (P("seq", "head"), P(None, "seq", "head"))
    return jax.shard_map(
        functools.partial(local, mesh.shape["seq"]),
        mesh=mesh,
        in_specs=in_specs,
        out_specs=out_specs,
        check_vma=False,
    )
```

```python
import functools

import jax
import jax.numpy as jnp
from jax import lax
from jax.experimental import pallas as pl
from jax.experimental.pallas import tpu as pltpu
from jax.sharding import PartitionSpec as P

HEAD_COUNT = 64
HDIM = 128
BLOCK = 256
PROMPTS = 4
PAIR = 2


EPSILON = 1e-06
MESH = pl.DeviceIdType.MESH


def fused_kernel(
    n,
    steps,
    query_ref,
    key_ref,
    value_ref,
    cols_ref,
    cum_ref,
    bias_ref,
    coef_ref,
    mask_ref,
    sq_ref,
    sk_ref,
    sv_ref,
    weight_ref,
    row_ref,
    mixed_ref,
    square_ref,
    dec_ref,
    dsquare_ref,
    own_part,
    x_send,
    x_recv,
    coef_recv,
    q_send,
    q_recv,
    row_recv,
    f_recv,
    f_send,
    b_recv,
    b_send,
    e_send,
    e_recv,
    r_send,
    r_recv,
    xs_sem,
    xr_sem,
    cs_sem,
    cr_sem,
    qs_sem,
    qr_sem,
    ws_sem,
    wr_sem,
    fs_sem,
    fr_sem,
    bs_sem,
    br_sem,
    es_sem,
    er_sem,
    rs_sem,
    rr_sem,
):
    f32, bf16 = jnp.float32, jnp.bfloat16
    me = lax.axis_index("seq")
    side = lax.rem(me, PAIR)
    rank = me // PAIR
    ranks = n // PAIR
    partner = me + 1 - 2 * side
    half, slots = own_part.shape[:2]
    rows = sq_ref.shape[0] // steps
    mine = side * half
    theirs = (1 - side) * half
    is_first = rank == 0
    is_last = rank == ranks - 1
    low = side == 0
    ahead = lax.rem(me + PAIR, n)
    behind = lax.rem(me + n - PAIR, n)

    def copy(src, dst, send, recv, to):
        return pltpu.make_async_remote_copy(
            src_ref=src,
            dst_ref=dst,
            send_sem=send,
            recv_sem=recv,
            device_id={"seq": to},
            device_id_type=MESH,
        )

    def x_copy(j, p):
        i = j * slots + p
        return copy(x_send.at[j, p], x_recv.at[j, p], xs_sem.at[i], xr_sem.at[i], partner)

    def f_copy(j, p):
        i = j * slots + p
        return copy(f_send.at[j, p], f_recv.at[j, p], fs_sem.at[i], fr_sem.at[i], ahead)

    def b_copy(j, p):
        i = j * slots + p
        return copy(b_send.at[j, p], b_recv.at[j, p], bs_sem.at[i], br_sem.at[i], behind)

    def q_copy(j):
        return copy(q_send.at[j], q_recv.at[j], qs_sem.at[j], qr_sem.at[j], partner)

    def e_copy(j):
        return copy(e_send.at[j], e_recv.at[j], es_sem.at[j], er_sem.at[j], partner)

    def r_copy(j):
        return copy(r_send.at[j], r_recv.at[j], rs_sem.at[j], rr_sem.at[j], partner)

    coef_copy = copy(coef_ref.at[pl.ds(theirs, half)], coef_recv, cs_sem, cr_sem, partner)
    row_copy = copy(row_ref, row_recv, ws_sem, wr_sem, partner)

    def lanes(h):
        return pl.ds(pl.multiple_of(h * HDIM, HDIM), HDIM)

    barrier = pltpu.get_barrier_semaphore()
    pl.semaphore_signal(barrier, inc=1, device_id={"seq": partner}, device_id_type=MESH)

    @pl.when(jnp.logical_not(is_last))
    def _():
        pl.semaphore_signal(barrier, inc=1, device_id={"seq": ahead}, device_id_type=MESH)

    @pl.when(jnp.logical_not(is_first))
    def _():
        pl.semaphore_signal(barrier, inc=1, device_id={"seq": behind}, device_id_type=MESH)

    def make_parts(h, j, into):
        key = key_ref[:, lanes(h)].astype(f32)
        value = value_ref[:, lanes(h)]
        for p in range(slots):
            keyed = (key * cols_ref[h, :, p : p + 1]).astype(bf16)
            into[j, p] = lax.dot_general(
                keyed, value, (((0,), (0,)), ((), ())), preferred_element_type=f32
            )

    def within(h):
        query = query_ref[:, lanes(h)]
        scores = lax.dot_general(
            query, key_ref[:, lanes(h)], (((1,), (1,)), ((), ())), preferred_element_type=f32
        )
        spread = cols_ref[h, :, slots : slots + 1] - cum_ref[h] + bias_ref[...]
        weights = (scores * jnp.exp(spread)).astype(bf16)
        mixed_ref[:, lanes(h)] = jnp.dot(
            weights, value_ref[:, lanes(h)], preferred_element_type=f32
        )

    def across(h, entry):
        carried = cols_ref[h, :, slots + 1 : slots + 2]
        outer = jnp.dot(query_ref[:, lanes(h)], entry.astype(bf16), preferred_element_type=f32)
        mixed = mixed_ref[:, lanes(h)] + outer * carried
        mixed_ref[:, lanes(h)] = mixed
        square_ref[...] += mixed * mixed

    def own_steps(h):
        query = sq_ref[:, lanes(h)].astype(f32)
        key = sk_ref[:, lanes(h)].astype(f32)
        value = sv_ref[:, lanes(h)].astype(f32)
        weight = weight_ref[h]
        cut = lambda a, i: a[i * rows : (i + 1) * rows]
        spot = 0
        for i in range(steps):
            total = None
            for j in range(i + 1):
                dot = jnp.sum(cut(query, i) * cut(key, j), axis=1, keepdims=True)
                term = dot * weight[:, spot : spot + 1] * cut(value, j)
                total = term if j == 0 else total + term
                spot += 1
            dec_ref[i * rows : (i + 1) * rows, lanes(h)] = total

    def from_state(h, product):
        weight = weight_ref[h]
        spot = steps * (steps + 1) // 2
        for i in range(steps):
            at = slice(i * rows, (i + 1) * rows)
            out = dec_ref[at, lanes(h)] + weight[:, spot + i : spot + i + 1] * product[at]
            dec_ref[at, lanes(h)] = out
            dsquare_ref[at] += out * out

    square_ref[...] = jnp.zeros_like(square_ref)
    dsquare_ref[...] = jnp.zeros_like(dsquare_ref)
    make_parts(theirs, 0, x_send)
    pl.semaphore_wait(barrier, 1 + jnp.where(is_first, 0, 1) + jnp.where(is_last, 0, 1))
    coef_copy.start()

    @pl.loop(0, half)
    def _(j):
        @pl.when(j > 0)
        def _():
            make_parts(theirs + j, j, x_send)

        for p in range(slots):
            x_copy(j, p).start()

        @pl.when(j == 0)
        def _():
            row_copy.start()

        q_send[j] = sq_ref[:, lanes(theirs + j)].astype(f32)
        q_copy(j).start()
        make_parts(mine + j, j, own_part)

    @pl.when(is_first)
    def _():
        f_recv[...] = jnp.zeros_like(f_recv)

    @pl.when(is_last)
    def _():
        b_recv[...] = jnp.zeros_like(b_recv)

    coef_copy.wait()
    row_copy.wait()

    lag = jnp.where(is_last, 0, ranks - rank)

    def forward(j):
        acc_mine = None
        acc_theirs = None
        for p in range(slots):
            x_copy(j, p).wait_recv()

            @pl.when(jnp.logical_not(is_first))
            def _():
                f_copy(j, p).wait_recv()

            own = own_part[j, p]
            other = x_recv[j, p]
            c_own = coef_ref[mine + j, pl.ds(p, 1), :]
            c_other = coef_recv[j, pl.ds(p, 1), :]
            came = f_recv[j, p]
            middle = jnp.where(low, c_own, c_other) * came + jnp.where(low, own, other)
            after = jnp.where(low, c_other, c_own) * middle + jnp.where(low, other, own)
            f_send[j, p] = after

            @pl.when(jnp.logical_not(is_last))
            def _():
                f_copy(j, p).start()

            at_low = came * mask_ref[pl.ds(p, 1), :]
            at_high = middle * mask_ref[pl.ds(slots + p, 1), :]
            to_mine = jnp.where(low, at_low, at_high)
            to_theirs = jnp.where(low, at_high, at_low)
            acc_mine = to_mine if p == 0 else acc_mine + to_mine
            acc_theirs = to_theirs if p == 0 else acc_theirs + to_theirs
        e_send[j] = acc_theirs
        e_copy(j).start()
        within(mine + j)
        across(mine + j, acc_mine)

    def backward(j):
        q_copy(j).wait_recv()
        q_own = sq_ref[:, lanes(mine + j)]
        q_other = q_recv[j].astype(bf16)
        total_own = None
        total_other = None
        for p in range(slots):

            @pl.when(jnp.logical_not(is_last))
            def _():
                b_copy(j, p).wait_recv()

            ended = mask_ref[pl.ds(2 * slots + p, 1), :]
            final = ended * f_send[j, p] + (1.0 - ended) * b_recv[j, p]
            b_send[j, p] = final

            @pl.when(jnp.logical_not(is_first))
            def _():
                b_copy(j, p).start()

            final_half = final.astype(bf16)
            got_own = jnp.dot(q_own, final_half, preferred_element_type=f32)
            got_other = jnp.dot(q_other, final_half, preferred_element_type=f32)
            got_own = jnp.where(row_ref[...] == float(p), got_own, 0.0)
            got_other = jnp.where(row_recv[...] == float(p), got_other, 0.0)
            total_own = got_own if p == 0 else total_own + got_own
            total_other = got_other if p == 0 else total_other + got_other
        r_send[j] = total_other
        r_copy(j).start()
        from_state(mine + j, total_own)

    @pl.loop(0, half + ranks)
    def _(t):
        @pl.when(t < half)
        def _():
            own_steps(t)
            own_steps(half + t)
            forward(t)

        @pl.when((t >= lag) & (t < half + lag))
        def _():
            backward(t - lag)

        @pl.when(t < half)
        def _():
            within(theirs + t)

    @pl.loop(0, half)
    def _(j):
        e_copy(j).wait()
        across(theirs + j, e_recv[j])

    @pl.loop(0, half)
    def _(j):
        r_copy(j).wait()
        from_state(theirs + j, r_recv[j])
        q_copy(j).wait_send()
        for p in range(slots):
            x_copy(j, p).wait_send()

            @pl.when(jnp.logical_not(is_last))
            def _():
                f_copy(j, p).wait_send()

            @pl.when(jnp.logical_not(is_first))
            def _():
                b_copy(j, p).wait_send()


def fused(n, steps, *operands):
    query, coef, step = operands[0], operands[6], operands[8]
    tok, width = query.shape
    heads, slots = coef.shape[:2]
    half = heads // PAIR
    vectors = step.shape[0]
    chunks = half * slots
    f32 = jnp.float32
    vmem = pl.BlockSpec(memory_space=pltpu.VMEM)
    dma = pltpu.SemaphoreType.DMA
    states = pltpu.VMEM((half, slots, HDIM, HDIM), f32)
    entries = pltpu.VMEM((half, HDIM, HDIM), f32)
    products = pltpu.VMEM((half, vectors, HDIM), f32)
    return pl.pallas_call(
        functools.partial(fused_kernel, n, steps),
        out_shape=(
            jax.ShapeDtypeStruct((tok, width), f32),
            jax.ShapeDtypeStruct((tok, HDIM), f32),
            jax.ShapeDtypeStruct((vectors, width), f32),
            jax.ShapeDtypeStruct((vectors, HDIM), f32),
        ),
        in_specs=[vmem] * len(operands),
        out_specs=(vmem,) * 4,
        scratch_shapes=[
            states,
            states,
            states,
            pltpu.VMEM((half,) + coef.shape[1:], f32),
            products,
            products,
            pltpu.VMEM((vectors, HDIM), f32),
            states,
            states,
            states,
            states,
            entries,
            entries,
            products,
            products,
            dma((chunks,)),
            dma((chunks,)),
            dma,
            dma,
            dma((half,)),
            dma((half,)),
            dma,
            dma,
            dma((chunks,)),
            dma((chunks,)),
            dma((chunks,)),
            dma((chunks,)),
            dma((half,)),
            dma((half,)),
            dma((half,)),
            dma((half,)),
        ],
        compiler_params=pltpu.CompilerParams(
            collective_id=0, has_side_effects=True, vmem_limit_bytes=56 * 1024 * 1024
        ),
        name="fused",
    )(*operands)


def segment_ids(prompt_lengths, positions):
    boundary = jnp.cumsum(prompt_lengths)
    return jnp.sum((positions[:, None] >= boundary[None, :]).astype(jnp.int32), axis=1)


def local(
    n,
    query_in,
    key_in,
    value_in,
    log_decay,
    norm_gain,
    prompt_lengths,
    step_query,
    step_key,
    step_value,
    step_decay,
    row_prompt,
):
    f32 = jnp.float32
    tok = query_in.shape[0]
    heads = log_decay.shape[1]
    steps, rows = step_query.shape[:2]
    place = lax.axis_index("seq")
    first = place * tok
    pair_first = (place // PAIR) * (PAIR * tok)
    ends = jnp.cumsum(prompt_lengths)
    begins = ends - prompt_lengths
    segs = segment_ids(prompt_lengths, first + jnp.arange(tok, dtype=jnp.int32))
    slot = jnp.arange(PROMPTS, dtype=jnp.int32)

    def seg_before(token):
        return jnp.where(token > 0, segment_ids(prompt_lengths, (token - 1)[None])[0], -1)

    seg_front = seg_before(first)
    cum = jnp.cumsum(log_decay, axis=0)

    last = jnp.clip(ends - first, 1, tok) - 1
    reached = jnp.sum(
        jnp.where((jnp.arange(tok)[None, :] == last[:, None])[:, :, None], cum[None], 0.0), axis=1
    )
    taken = (segs[None, :] == slot[:, None])[:, :, None]
    keep = jnp.where(taken, jnp.exp(jnp.where(taken, reached[:, None, :] - cum[None], 0.0)), 0.0)
    carried = jnp.exp(cum) * (segs == seg_front).astype(f32)[:, None]
    cols = jnp.transpose(jnp.concatenate([keep, cum[None], carried[None]]), (2, 1, 0))
    cum_rows = cum.T[:, None, :]
    causal = jnp.arange(tok)[:, None] >= jnp.arange(tok)[None, :]
    linked = causal & (segs[:, None] == segs[None, :])
    bias = jnp.where(linked, 0.0, -jnp.inf)
    coef = jnp.where(
        (ends <= first)[:, None], 1.0, jnp.where((begins < first)[:, None], jnp.exp(reached), 0.0)
    )
    coef = jnp.broadcast_to(coef.T[:, :, None], (heads, PROMPTS, HDIM))
    pair_last = pair_first + PAIR * tok
    marks = jnp.concatenate(
        [slot == seg_before(pair_first), slot == seg_before(pair_first + tok), ends <= pair_last]
    )
    marks = jnp.concatenate([marks, jnp.zeros((4,), bool)])
    masks = jnp.broadcast_to(marks.astype(f32)[:, None], (marks.shape[0], HDIM))

    shares, wholes = [], []
    for i in range(steps):
        for j in range(i + 1):
            shares.append(jnp.exp(jnp.sum(step_decay[j + 1 : i + 1], axis=0)))
        wholes.append(jnp.exp(jnp.sum(step_decay[: i + 1], axis=0)))
    step_weights = jnp.transpose(jnp.stack(shares + wholes), (2, 1, 0))
    row_marks = jnp.broadcast_to(
        jnp.broadcast_to(row_prompt.astype(f32)[None, :], (steps, rows)).reshape(-1, 1),
        (steps * rows, HDIM),
    )
    flat = lambda a: a.reshape(steps * rows, -1)
    mixed, mixed_sq, decoded, decoded_sq = fused(
        n,
        steps,
        query_in,
        key_in,
        value_in,
        cols,
        cum_rows,
        bias,
        coef,
        masks,
        flat(step_query),
        flat(step_key),
        flat(step_value),
        step_weights,
        row_marks,
    )
    squares, step_squares = lax.psum(
        (jnp.sum(mixed_sq, axis=1), jnp.sum(decoded_sq, axis=1)), "head"
    )
    scale = lax.rsqrt(squares / (HEAD_COUNT * HDIM) + EPSILON)
    attn_out = (mixed * scale[:, None] * norm_gain[None, :]).astype(jnp.bfloat16)
    step_scale = lax.rsqrt(step_squares / (HEAD_COUNT * HDIM) + EPSILON)
    decode_out = (decoded * step_scale[:, None] * norm_gain[None, :]).astype(jnp.bfloat16)
    return (attn_out, decode_out.reshape(step_query.shape))


def solution(mesh):
    in_specs = (
        P("seq", "head"),
        P("seq", "head"),
        P("seq", "head"),
        P("seq", "head"),
        P("head"),
        P(),
        P(None, "seq", "head"),
        P(None, "seq", "head"),
        P(None, "seq", "head"),
        P(None, "seq", "head"),
        P("seq"),
    )
    out_specs = (P("seq", "head"), P(None, "seq", "head"))
    return jax.shard_map(
        functools.partial(local, mesh.shape["seq"]),
        mesh=mesh,
        in_specs=in_specs,
        out_specs=out_specs,
        check_vma=False,
    )
```

```python
import functools

import jax
import jax.numpy as jnp
from jax import lax
from jax.experimental import pallas as pl
from jax.experimental.pallas import tpu as pltpu
from jax.sharding import PartitionSpec as P

HEAD_COUNT = 64
HDIM = 128
BLOCK = 256
PROMPTS = 4
PAIR = 2


EPSILON = 1e-06
MESH = pl.DeviceIdType.MESH


def fused_kernel(
    n,
    steps,
    query_ref,
    key_ref,
    value_ref,
    cols_ref,
    cum_ref,
    bias_ref,
    coef_ref,
    mask_ref,
    sq_ref,
    sk_ref,
    sv_ref,
    weight_ref,
    row_ref,
    mixed_ref,
    square_ref,
    dec_ref,
    dsquare_ref,
    own_part,
    x_send,
    x_recv,
    coef_recv,
    q_send,
    q_recv,
    row_recv,
    f_recv,
    f_send,
    b_recv,
    b_send,
    pair_part,
    t_recv,
    t_send,
    e_mine,
    acc_sq,
    acc_dsq,
    e_send,
    e_recv,
    r_send,
    r_recv,
    xs_sem,
    xr_sem,
    cs_sem,
    cr_sem,
    qs_sem,
    qr_sem,
    ws_sem,
    wr_sem,
    fs_sem,
    fr_sem,
    bs_sem,
    br_sem,
    ts_sem,
    tr_sem,
    es_sem,
    er_sem,
    rs_sem,
    rr_sem,
):
    f32, bf16 = jnp.float32, jnp.bfloat16
    me = lax.axis_index("seq")
    side = lax.rem(me, PAIR)
    rank = me // PAIR
    ranks = n // PAIR
    partner = me + 1 - 2 * side
    half, slots = own_part.shape[:2]
    rows = sq_ref.shape[0] // steps
    mine = side * half
    theirs = (1 - side) * half
    is_first = rank == 0
    is_last = rank == ranks - 1
    low = side == 0
    ahead = lax.rem(me + PAIR, n)
    behind = lax.rem(me + n - PAIR, n)

    def copy(src, dst, send, recv, to):
        return pltpu.make_async_remote_copy(
            src_ref=src,
            dst_ref=dst,
            send_sem=send,
            recv_sem=recv,
            device_id={"seq": to},
            device_id_type=MESH,
        )

    def x_copy(j, p):
        i = j * slots + p
        return copy(x_send.at[j, p], x_recv.at[j, p], xs_sem.at[i], xr_sem.at[i], partner)

    def f_copy(j, p):
        i = j * slots + p
        return copy(f_send.at[j, p], f_recv.at[j, p], fs_sem.at[i], fr_sem.at[i], ahead)

    def b_copy(j, p):
        i = j * slots + p
        return copy(b_send.at[j, p], b_recv.at[j, p], bs_sem.at[i], br_sem.at[i], behind)

    def q_copy(j):
        return copy(q_send.at[j], q_recv.at[j], qs_sem.at[j], qr_sem.at[j], partner)

    def e_copy(j):
        return copy(e_send.at[j], e_recv.at[j], es_sem.at[j], er_sem.at[j], partner)

    def r_copy(j):
        return copy(r_send.at[j], r_recv.at[j], rs_sem.at[j], rr_sem.at[j], partner)

    coef_copy = copy(coef_ref.at[pl.ds(theirs, half)], coef_recv, cs_sem, cr_sem, partner)
    row_copy = copy(row_ref, row_recv, ws_sem, wr_sem, partner)

    t_copy = copy(t_send, t_recv, ts_sem, tr_sem, behind)

    def lanes(h):
        return pl.ds(pl.multiple_of(h * HDIM, HDIM), HDIM)

    barrier = pltpu.get_barrier_semaphore()
    pl.semaphore_signal(barrier, inc=1, device_id={"seq": partner}, device_id_type=MESH)

    @pl.when(jnp.logical_not(is_last))
    def _():
        pl.semaphore_signal(barrier, inc=1, device_id={"seq": ahead}, device_id_type=MESH)

    @pl.when(jnp.logical_not(is_first))
    def _():
        pl.semaphore_signal(barrier, inc=1, device_id={"seq": behind}, device_id_type=MESH)

    def make_parts(h, j, into):
        key = key_ref[:, lanes(h)].astype(f32)
        value = value_ref[:, lanes(h)]
        for p in range(slots):
            keyed = (key * cols_ref[h, :, p : p + 1]).astype(bf16)
            into[j, p] = lax.dot_general(
                keyed, value, (((0,), (0,)), ((), ())), preferred_element_type=f32
            )

    def within(h):
        query = query_ref[:, lanes(h)]
        scores = lax.dot_general(
            query, key_ref[:, lanes(h)], (((1,), (1,)), ((), ())), preferred_element_type=f32
        )
        spread = cols_ref[h, :, slots : slots + 1] - cum_ref[h] + bias_ref[...]
        weights = (scores * jnp.exp(spread)).astype(bf16)
        mixed_ref[:, lanes(h)] = jnp.dot(
            weights, value_ref[:, lanes(h)], preferred_element_type=f32
        )

    def across(h, entry):
        carried = cols_ref[h, :, slots + 1 : slots + 2]
        outer = jnp.dot(query_ref[:, lanes(h)], entry.astype(bf16), preferred_element_type=f32)
        mixed = mixed_ref[:, lanes(h)] + outer * carried
        mixed_ref[:, lanes(h)] = mixed
        acc_sq[...] += mixed * mixed

    def own_steps(h):
        query = sq_ref[:, lanes(h)].astype(f32)
        key = sk_ref[:, lanes(h)].astype(f32)
        value = sv_ref[:, lanes(h)].astype(f32)
        weight = weight_ref[h]
        cut = lambda a, i: a[i * rows : (i + 1) * rows]
        spot = 0
        for i in range(steps):
            total = None
            for j in range(i + 1):
                dot = jnp.sum(cut(query, i) * cut(key, j), axis=1, keepdims=True)
                term = dot * weight[:, spot : spot + 1] * cut(value, j)
                total = term if j == 0 else total + term
                spot += 1
            dec_ref[i * rows : (i + 1) * rows, lanes(h)] = total

    def from_state(h, product):
        weight = weight_ref[h]
        spot = steps * (steps + 1) // 2
        for i in range(steps):
            at = slice(i * rows, (i + 1) * rows)
            out = dec_ref[at, lanes(h)] + weight[:, spot + i : spot + i + 1] * product[at]
            dec_ref[at, lanes(h)] = out
            acc_dsq[at] += out * out

    acc_sq[...] = jnp.zeros_like(acc_sq)
    acc_dsq[...] = jnp.zeros_like(acc_dsq)
    make_parts(theirs, 0, x_send)
    pl.semaphore_wait(barrier, 1 + jnp.where(is_first, 0, 1) + jnp.where(is_last, 0, 1))
    coef_copy.start()

    @pl.loop(0, half)
    def _(j):
        @pl.when(j > 0)
        def _():
            make_parts(theirs + j, j, x_send)

        for p in range(slots):
            x_copy(j, p).start()

        @pl.when(j == 0)
        def _():
            row_copy.start()

        q_send[j] = sq_ref[:, lanes(theirs + j)].astype(f32)
        q_copy(j).start()
        make_parts(mine + j, j, own_part)

    @pl.when(is_first)
    def _():
        f_recv[...] = jnp.zeros_like(f_recv)

    @pl.when(is_last)
    def _():
        b_recv[...] = jnp.zeros_like(b_recv)

    coef_copy.wait()
    row_copy.wait()

    @pl.when(is_last)
    def _():
        t_recv[...] = jnp.ones_like(t_recv)

    lag_f = rank
    lag_b = ranks - 1 - rank
    lag_d = jnp.maximum(lag_f, lag_b)

    def relay_decay():
        @pl.when(jnp.logical_not(is_last))
        def _():
            t_copy.wait_recv()

        @pl.when(jnp.logical_not(is_first))
        def _():
            t_send[...] = t_recv[...] * coef_recv[...] * coef_ref[pl.ds(mine, half)]
            t_copy.start()

    def rows_of(j, p):
        c_own = coef_ref[mine + j, pl.ds(p, 1), :]
        c_other = coef_recv[j, pl.ds(p, 1), :]
        return jnp.where(low, c_own, c_other), jnp.where(low, c_other, c_own)

    def combine(j):
        for p in range(slots):
            x_copy(j, p).wait_recv()
            own = own_part[j, p]
            other = x_recv[j, p]
            c_low, c_high = rows_of(j, p)
            pair = c_high * jnp.where(low, own, other) + jnp.where(low, other, own)
            pair_part[j, p] = pair

            @pl.when(is_first)
            def _():
                f_send[j, p] = pair

                @pl.when(jnp.logical_not(is_last))
                def _():
                    f_copy(j, p).start()

            @pl.when(is_last & jnp.logical_not(is_first))
            def _():
                b_send[j, p] = pair
                b_copy(j, p).start()

    def forward(j):
        acc_mine = None
        acc_theirs = None
        for p in range(slots):
            c_low, c_high = rows_of(j, p)

            @pl.when(jnp.logical_not(is_first))
            def _():
                f_copy(j, p).wait_recv()
                f_send[j, p] = (c_low * c_high) * f_recv[j, p] + pair_part[j, p]

                @pl.when(jnp.logical_not(is_last))
                def _():
                    f_copy(j, p).start()

            came = f_recv[j, p]
            middle = c_low * came + jnp.where(low, own_part[j, p], x_recv[j, p])
            at_low = came * mask_ref[pl.ds(p, 1), :]
            at_high = middle * mask_ref[pl.ds(slots + p, 1), :]
            to_mine = jnp.where(low, at_low, at_high)
            to_theirs = jnp.where(low, at_high, at_low)
            acc_mine = to_mine if p == 0 else acc_mine + to_mine
            acc_theirs = to_theirs if p == 0 else acc_theirs + to_theirs
        e_send[j] = acc_theirs
        e_copy(j).start()
        e_mine[j] = acc_mine

    def backward(j):
        for p in range(slots):

            @pl.when(jnp.logical_not(is_last))
            def _():
                b_copy(j, p).wait_recv()

                @pl.when(jnp.logical_not(is_first))
                def _():
                    b_send[j, p] = b_recv[j, p] + t_recv[j, pl.ds(p, 1), :] * pair_part[j, p]
                    b_copy(j, p).start()

    def decode(j):
        q_copy(j).wait_recv()
        q_own = sq_ref[:, lanes(mine + j)]
        q_other = q_recv[j].astype(bf16)
        total_own = None
        total_other = None
        for p in range(slots):
            final = t_recv[j, pl.ds(p, 1), :] * f_send[j, p] + b_recv[j, p]
            final_half = final.astype(bf16)
            got_own = jnp.dot(q_own, final_half, preferred_element_type=f32)
            got_other = jnp.dot(q_other, final_half, preferred_element_type=f32)
            got_own = jnp.where(row_ref[...] == float(p), got_own, 0.0)
            got_other = jnp.where(row_recv[...] == float(p), got_other, 0.0)
            total_own = got_own if p == 0 else total_own + got_own
            total_other = got_other if p == 0 else total_other + got_other
        r_send[j] = total_other
        r_copy(j).start()
        from_state(mine + j, total_own)

    @pl.loop(0, half + ranks - 1)
    def _(t):
        @pl.when(t < half)
        def _():
            own_steps(t)
            own_steps(half + t)
            within(mine + t)
            within(theirs + t)

        @pl.when(t == lag_b)
        def _():
            relay_decay()

        @pl.when(t < half)
        def _():
            combine(t)

        @pl.when((t >= lag_f) & (t < half + lag_f))
        def _():
            forward(t - lag_f)

        @pl.when((t >= lag_b) & (t < half + lag_b))
        def _():
            backward(t - lag_b)

        @pl.when((t >= lag_d) & (t < half + lag_d))
        def _():
            decode(t - lag_d)

        @pl.when((t >= lag_f) & (t < half + lag_f))
        def _():
            across(mine + t - lag_f, e_mine[t - lag_f])

    @pl.loop(0, half)
    def _(j):
        e_copy(j).wait()
        across(theirs + j, e_recv[j])

    @pl.loop(0, half)
    def _(j):
        r_copy(j).wait()
        from_state(theirs + j, r_recv[j])
        q_copy(j).wait_send()
        for p in range(slots):
            x_copy(j, p).wait_send()

            @pl.when(jnp.logical_not(is_last))
            def _():
                f_copy(j, p).wait_send()

            @pl.when(jnp.logical_not(is_first))
            def _():
                b_copy(j, p).wait_send()

    @pl.when(jnp.logical_not(is_first))
    def _():
        t_copy.wait_send()

    square_ref[...] = jnp.sum(acc_sq[...], axis=1, keepdims=True)
    dsquare_ref[...] = jnp.sum(acc_dsq[...], axis=1, keepdims=True)


def fused(n, steps, *operands):
    query, coef, step = operands[0], operands[6], operands[8]
    tok, width = query.shape
    heads, slots = coef.shape[:2]
    half = heads // PAIR
    vectors = step.shape[0]
    chunks = half * slots
    f32 = jnp.float32
    vmem = pl.BlockSpec(memory_space=pltpu.VMEM)
    dma = pltpu.SemaphoreType.DMA
    states = pltpu.VMEM((half, slots, HDIM, HDIM), f32)
    decays = pltpu.VMEM((half,) + coef.shape[1:], f32)
    entries = pltpu.VMEM((half, HDIM, HDIM), f32)
    products = pltpu.VMEM((half, vectors, HDIM), f32)
    return pl.pallas_call(
        functools.partial(fused_kernel, n, steps),
        out_shape=(
            jax.ShapeDtypeStruct((tok, width), f32),
            jax.ShapeDtypeStruct((tok, 1), f32),
            jax.ShapeDtypeStruct((vectors, width), f32),
            jax.ShapeDtypeStruct((vectors, 1), f32),
        ),
        in_specs=[vmem] * len(operands),
        out_specs=(vmem,) * 4,
        scratch_shapes=[
            states,
            states,
            states,
            decays,
            products,
            products,
            pltpu.VMEM((vectors, HDIM), f32),
            states,
            states,
            states,
            states,
            states,
            decays,
            decays,
            entries,
            pltpu.VMEM((tok, HDIM), f32),
            pltpu.VMEM((vectors, HDIM), f32),
            entries,
            entries,
            products,
            products,
            dma((chunks,)),
            dma((chunks,)),
            dma,
            dma,
            dma((half,)),
            dma((half,)),
            dma,
            dma,
            dma((chunks,)),
            dma((chunks,)),
            dma((chunks,)),
            dma((chunks,)),
            dma,
            dma,
            dma((half,)),
            dma((half,)),
            dma((half,)),
            dma((half,)),
        ],
        compiler_params=pltpu.CompilerParams(
            collective_id=0, has_side_effects=True, vmem_limit_bytes=56 * 1024 * 1024
        ),
        name="fused",
    )(*operands)


def segment_ids(prompt_lengths, positions):
    boundary = jnp.cumsum(prompt_lengths)
    return jnp.sum((positions[:, None] >= boundary[None, :]).astype(jnp.int32), axis=1)


def local(
    n,
    query_in,
    key_in,
    value_in,
    log_decay,
    norm_gain,
    prompt_lengths,
    step_query,
    step_key,
    step_value,
    step_decay,
    row_prompt,
):
    f32 = jnp.float32
    tok = query_in.shape[0]
    heads = log_decay.shape[1]
    steps, rows = step_query.shape[:2]
    place = lax.axis_index("seq")
    first = place * tok
    pair_first = (place // PAIR) * (PAIR * tok)
    ends = jnp.cumsum(prompt_lengths)
    begins = ends - prompt_lengths
    segs = segment_ids(prompt_lengths, first + jnp.arange(tok, dtype=jnp.int32))
    slot = jnp.arange(PROMPTS, dtype=jnp.int32)

    def seg_before(token):
        return jnp.where(token > 0, segment_ids(prompt_lengths, (token - 1)[None])[0], -1)

    seg_front = seg_before(first)
    cum = jnp.cumsum(log_decay, axis=0)

    last = jnp.clip(ends - first, 1, tok) - 1
    reached = jnp.sum(
        jnp.where((jnp.arange(tok)[None, :] == last[:, None])[:, :, None], cum[None], 0.0), axis=1
    )
    taken = (segs[None, :] == slot[:, None])[:, :, None]
    keep = jnp.where(taken, jnp.exp(jnp.where(taken, reached[:, None, :] - cum[None], 0.0)), 0.0)
    carried = jnp.exp(cum) * (segs == seg_front).astype(f32)[:, None]
    cols = jnp.transpose(jnp.concatenate([keep, cum[None], carried[None]]), (2, 1, 0))
    cum_rows = cum.T[:, None, :]
    causal = jnp.arange(tok)[:, None] >= jnp.arange(tok)[None, :]
    linked = causal & (segs[:, None] == segs[None, :])
    bias = jnp.where(linked, 0.0, -jnp.inf)
    coef = jnp.where(
        (ends <= first)[:, None], 1.0, jnp.where((begins < first)[:, None], jnp.exp(reached), 0.0)
    )
    coef = jnp.broadcast_to(coef.T[:, :, None], (heads, PROMPTS, HDIM))
    pair_last = pair_first + PAIR * tok
    marks = jnp.concatenate(
        [slot == seg_before(pair_first), slot == seg_before(pair_first + tok), ends <= pair_last]
    )
    marks = jnp.concatenate([marks, jnp.zeros((4,), bool)])
    masks = jnp.broadcast_to(marks.astype(f32)[:, None], (marks.shape[0], HDIM))

    shares = [
        [float(j < k <= i) for k in range(steps)] for i in range(steps) for j in range(i + 1)
    ]
    wholes = [[float(k <= i) for k in range(steps)] for i in range(steps)]
    step_weights = jnp.exp(
        jnp.einsum(
            "irh,wi->hrw", step_decay, jnp.array(shares + wholes, f32), precision=lax.Precision.HIGHEST
        )
    )
    row_marks = jnp.broadcast_to(
        jnp.broadcast_to(row_prompt.astype(f32)[None, :], (steps, rows)).reshape(-1, 1),
        (steps * rows, HDIM),
    )
    flat = lambda a: a.reshape(steps * rows, -1)
    mixed, mixed_sq, decoded, decoded_sq = fused(
        n,
        steps,
        query_in,
        key_in,
        value_in,
        cols,
        cum_rows,
        bias,
        coef,
        masks,
        flat(step_query),
        flat(step_key),
        flat(step_value),
        step_weights,
        row_marks,
    )
    squares, step_squares = lax.psum(
        (mixed_sq[:, 0], decoded_sq[:, 0]), "head"
    )
    scale = lax.rsqrt(squares / (HEAD_COUNT * HDIM) + EPSILON)
    attn_out = (mixed * scale[:, None] * norm_gain[None, :]).astype(jnp.bfloat16)
    step_scale = lax.rsqrt(step_squares / (HEAD_COUNT * HDIM) + EPSILON)
    decode_out = (decoded * step_scale[:, None] * norm_gain[None, :]).astype(jnp.bfloat16)
    return (attn_out, decode_out.reshape(step_query.shape))


def solution(mesh):
    in_specs = (
        P("seq", "head"),
        P("seq", "head"),
        P("seq", "head"),
        P("seq", "head"),
        P("head"),
        P(),
        P(None, "seq", "head"),
        P(None, "seq", "head"),
        P(None, "seq", "head"),
        P(None, "seq", "head"),
        P("seq"),
    )
    out_specs = (P("seq", "head"), P(None, "seq", "head"))
    return jax.shard_map(
        functools.partial(local, mesh.shape["seq"]),
        mesh=mesh,
        in_specs=in_specs,
        out_specs=out_specs,
        check_vma=False,
    )
```

```python
import functools

import jax
import jax.numpy as jnp
from jax import lax
from jax.experimental import pallas as pl
from jax.experimental.pallas import tpu as pltpu
from jax.sharding import PartitionSpec as P

HEAD_COUNT = 64
HDIM = 128
BLOCK = 256
PROMPTS = 4
PAIR = 2


EPSILON = 1e-06
MESH = pl.DeviceIdType.MESH


def fused_kernel(
    n,
    steps,
    query_ref,
    key_ref,
    value_ref,
    token_ref,
    bias_ref,
    coef_ref,
    mask_ref,
    sq_ref,
    sk_ref,
    sv_ref,
    weight_ref,
    row_ref,
    mixed_ref,
    square_ref,
    dec_ref,
    dsquare_ref,
    own_part,
    x_send,
    x_recv,
    coef_recv,
    q_send,
    q_recv,
    row_recv,
    f_recv,
    f_send,
    b_recv,
    b_send,
    pair_part,
    t_recv,
    t_send,
    e_mine,
    acc_sq,
    acc_dsq,
    e_send,
    e_recv,
    r_send,
    r_recv,
    xs_sem,
    xr_sem,
    cs_sem,
    cr_sem,
    qs_sem,
    qr_sem,
    ws_sem,
    wr_sem,
    fs_sem,
    fr_sem,
    bs_sem,
    br_sem,
    ts_sem,
    tr_sem,
    es_sem,
    er_sem,
    rs_sem,
    rr_sem,
):
    f32, bf16 = jnp.float32, jnp.bfloat16
    me = lax.axis_index("seq")
    side = lax.rem(me, PAIR)
    rank = me // PAIR
    ranks = n // PAIR
    partner = me + 1 - 2 * side
    half, slots = own_part.shape[:2]
    rows = sq_ref.shape[0] // steps
    mine = side * half
    theirs = (1 - side) * half
    is_first = rank == 0
    is_last = rank == ranks - 1
    low = side == 0
    ahead = lax.rem(me + PAIR, n)
    behind = lax.rem(me + n - PAIR, n)

    def copy(src, dst, send, recv, to):
        return pltpu.make_async_remote_copy(
            src_ref=src,
            dst_ref=dst,
            send_sem=send,
            recv_sem=recv,
            device_id={"seq": to},
            device_id_type=MESH,
        )

    def x_copy(j, p):
        i = j * slots + p
        return copy(x_send.at[j, p], x_recv.at[j, p], xs_sem.at[i], xr_sem.at[i], partner)

    def f_copy(j, p):
        i = j * slots + p
        return copy(f_send.at[j, p], f_recv.at[j, p], fs_sem.at[i], fr_sem.at[i], ahead)

    def b_copy(j, p):
        i = j * slots + p
        return copy(b_send.at[j, p], b_recv.at[j, p], bs_sem.at[i], br_sem.at[i], behind)

    def q_copy(j):
        return copy(q_send.at[j], q_recv.at[j], qs_sem.at[j], qr_sem.at[j], partner)

    def e_copy(j):
        return copy(e_send.at[j], e_recv.at[j], es_sem.at[j], er_sem.at[j], partner)

    def r_copy(j):
        return copy(r_send.at[j], r_recv.at[j], rs_sem.at[j], rr_sem.at[j], partner)

    coef_copy = copy(coef_ref.at[pl.ds(theirs, half)], coef_recv, cs_sem, cr_sem, partner)
    row_copy = copy(row_ref, row_recv, ws_sem, wr_sem, partner)

    t_copy = copy(t_send, t_recv, ts_sem, tr_sem, behind)

    def lanes(h):
        return pl.ds(pl.multiple_of(h * HDIM, HDIM), HDIM)

    barrier = pltpu.get_barrier_semaphore()
    pl.semaphore_signal(barrier, inc=1, device_id={"seq": partner}, device_id_type=MESH)

    @pl.when(jnp.logical_not(is_last))
    def _():
        pl.semaphore_signal(barrier, inc=1, device_id={"seq": ahead}, device_id_type=MESH)

    @pl.when(jnp.logical_not(is_first))
    def _():
        pl.semaphore_signal(barrier, inc=1, device_id={"seq": behind}, device_id_type=MESH)

    def make_parts(h, j, into):
        key = key_ref[:, lanes(h)].astype(f32)
        value = value_ref[:, lanes(h)]
        cols = jnp.transpose(token_ref[h])
        for p in range(slots):
            keyed = (key * cols[:, p : p + 1]).astype(bf16)
            into[j, p] = lax.dot_general(
                keyed, value, (((0,), (0,)), ((), ())), preferred_element_type=f32
            )

    def within(h):
        query = query_ref[:, lanes(h)]
        scores = lax.dot_general(
            query, key_ref[:, lanes(h)], (((1,), (1,)), ((), ())), preferred_element_type=f32
        )
        cols = jnp.transpose(token_ref[h])
        spread = cols[:, slots : slots + 1] - token_ref[h, slots : slots + 1, :] + bias_ref[...]
        weights = (scores * jnp.exp(spread)).astype(bf16)
        mixed_ref[:, lanes(h)] = jnp.dot(
            weights, value_ref[:, lanes(h)], preferred_element_type=f32
        )

    def across(h, entry):
        carried = jnp.transpose(token_ref[h])[:, slots + 1 : slots + 2]
        outer = jnp.dot(query_ref[:, lanes(h)], entry.astype(bf16), preferred_element_type=f32)
        mixed = mixed_ref[:, lanes(h)] + outer * carried
        mixed_ref[:, lanes(h)] = mixed
        acc_sq[...] += mixed * mixed

    def own_steps(h):
        query = sq_ref[:, lanes(h)].astype(f32)
        key = sk_ref[:, lanes(h)].astype(f32)
        value = sv_ref[:, lanes(h)].astype(f32)
        weight = weight_ref[h]
        cut = lambda a, i: a[i * rows : (i + 1) * rows]
        spot = 0
        for i in range(steps):
            total = None
            for j in range(i + 1):
                dot = jnp.sum(cut(query, i) * cut(key, j), axis=1, keepdims=True)
                term = dot * weight[:, spot : spot + 1] * cut(value, j)
                total = term if j == 0 else total + term
                spot += 1
            dec_ref[i * rows : (i + 1) * rows, lanes(h)] = total

    def from_state(h, product):
        weight = weight_ref[h]
        spot = steps * (steps + 1) // 2
        for i in range(steps):
            at = slice(i * rows, (i + 1) * rows)
            out = dec_ref[at, lanes(h)] + weight[:, spot + i : spot + i + 1] * product[at]
            dec_ref[at, lanes(h)] = out
            acc_dsq[at] += out * out

    acc_sq[...] = jnp.zeros_like(acc_sq)
    acc_dsq[...] = jnp.zeros_like(acc_dsq)
    make_parts(theirs, 0, x_send)
    pl.semaphore_wait(barrier, 1 + jnp.where(is_first, 0, 1) + jnp.where(is_last, 0, 1))
    coef_copy.start()

    @pl.loop(0, half)
    def _(j):
        @pl.when(j > 0)
        def _():
            make_parts(theirs + j, j, x_send)

        for p in range(slots):
            x_copy(j, p).start()

        @pl.when(j == 0)
        def _():
            row_copy.start()

        q_send[j] = sq_ref[:, lanes(theirs + j)].astype(f32)
        q_copy(j).start()
        make_parts(mine + j, j, own_part)

    @pl.when(is_first)
    def _():
        f_recv[...] = jnp.zeros_like(f_recv)

    @pl.when(is_last)
    def _():
        b_recv[...] = jnp.zeros_like(b_recv)

    coef_copy.wait()
    row_copy.wait()

    @pl.when(is_last)
    def _():
        t_recv[...] = jnp.ones_like(t_recv)

    lag_f = rank
    lag_b = ranks - 1 - rank
    lag_d = jnp.maximum(lag_f, lag_b)

    def relay_decay():
        @pl.when(jnp.logical_not(is_last))
        def _():
            t_copy.wait_recv()

        @pl.when(jnp.logical_not(is_first))
        def _():
            t_send[...] = t_recv[...] * coef_recv[...] * coef_ref[pl.ds(mine, half)]
            t_copy.start()

    def rows_of(j, p):
        c_own = coef_ref[mine + j, pl.ds(p, 1), :]
        c_other = coef_recv[j, pl.ds(p, 1), :]
        return jnp.where(low, c_own, c_other), jnp.where(low, c_other, c_own)

    def combine(j):
        for p in range(slots):
            x_copy(j, p).wait_recv()
            own = own_part[j, p]
            other = x_recv[j, p]
            c_low, c_high = rows_of(j, p)
            pair = c_high * jnp.where(low, own, other) + jnp.where(low, other, own)
            pair_part[j, p] = pair

            @pl.when(is_first)
            def _():
                f_send[j, p] = pair

                @pl.when(jnp.logical_not(is_last))
                def _():
                    f_copy(j, p).start()

            @pl.when(is_last & jnp.logical_not(is_first))
            def _():
                b_send[j, p] = pair
                b_copy(j, p).start()

    def forward(j):
        acc_mine = None
        acc_theirs = None
        for p in range(slots):
            c_low, c_high = rows_of(j, p)

            @pl.when(jnp.logical_not(is_first))
            def _():
                f_copy(j, p).wait_recv()
                f_send[j, p] = (c_low * c_high) * f_recv[j, p] + pair_part[j, p]

                @pl.when(jnp.logical_not(is_last))
                def _():
                    f_copy(j, p).start()

            came = f_recv[j, p]
            middle = c_low * came + jnp.where(low, own_part[j, p], x_recv[j, p])
            at_low = came * mask_ref[pl.ds(p, 1), :]
            at_high = middle * mask_ref[pl.ds(slots + p, 1), :]
            to_mine = jnp.where(low, at_low, at_high)
            to_theirs = jnp.where(low, at_high, at_low)
            acc_mine = to_mine if p == 0 else acc_mine + to_mine
            acc_theirs = to_theirs if p == 0 else acc_theirs + to_theirs
        e_send[j] = acc_theirs
        e_copy(j).start()
        e_mine[j] = acc_mine

    def backward(j):
        for p in range(slots):

            @pl.when(jnp.logical_not(is_last))
            def _():
                b_copy(j, p).wait_recv()

                @pl.when(jnp.logical_not(is_first))
                def _():
                    b_send[j, p] = b_recv[j, p] + t_recv[j, pl.ds(p, 1), :] * pair_part[j, p]
                    b_copy(j, p).start()

    def decode(j):
        q_copy(j).wait_recv()
        q_own = sq_ref[:, lanes(mine + j)]
        q_other = q_recv[j].astype(bf16)
        total_own = None
        total_other = None
        for p in range(slots):
            final = t_recv[j, pl.ds(p, 1), :] * f_send[j, p] + b_recv[j, p]
            final_half = final.astype(bf16)
            got_own = jnp.dot(q_own, final_half, preferred_element_type=f32)
            got_other = jnp.dot(q_other, final_half, preferred_element_type=f32)
            got_own = jnp.where(row_ref[...] == float(p), got_own, 0.0)
            got_other = jnp.where(row_recv[...] == float(p), got_other, 0.0)
            total_own = got_own if p == 0 else total_own + got_own
            total_other = got_other if p == 0 else total_other + got_other
        r_send[j] = total_other
        r_copy(j).start()
        from_state(mine + j, total_own)

    @pl.loop(0, half + ranks - 1)
    def _(t):
        @pl.when(t < half)
        def _():
            own_steps(t)
            own_steps(half + t)
            within(mine + t)
            within(theirs + t)

        @pl.when(t == lag_b)
        def _():
            relay_decay()

        @pl.when(t < half)
        def _():
            combine(t)

        @pl.when((t >= lag_f) & (t < half + lag_f))
        def _():
            forward(t - lag_f)

        @pl.when((t >= lag_b) & (t < half + lag_b))
        def _():
            backward(t - lag_b)

        @pl.when((t >= lag_d) & (t < half + lag_d))
        def _():
            decode(t - lag_d)

        @pl.when((t >= lag_f) & (t < half + lag_f))
        def _():
            across(mine + t - lag_f, e_mine[t - lag_f])

    @pl.loop(0, half)
    def _(j):
        e_copy(j).wait()
        across(theirs + j, e_recv[j])

    @pl.loop(0, half)
    def _(j):
        r_copy(j).wait()
        from_state(theirs + j, r_recv[j])
        q_copy(j).wait_send()
        for p in range(slots):
            x_copy(j, p).wait_send()

            @pl.when(jnp.logical_not(is_last))
            def _():
                f_copy(j, p).wait_send()

            @pl.when(jnp.logical_not(is_first))
            def _():
                b_copy(j, p).wait_send()

    @pl.when(jnp.logical_not(is_first))
    def _():
        t_copy.wait_send()

    def row_sums(acc):
        return lax.dot_general(
            jnp.ones((8, HDIM), f32),
            acc[...],
            (((1,), (1,)), ((), ())),
            precision=lax.Precision.HIGHEST,
            preferred_element_type=f32,
        )

    square_ref[...] = row_sums(acc_sq)
    dsquare_ref[...] = row_sums(acc_dsq)


def fused(n, steps, *operands):
    query, coef, step = operands[0], operands[5], operands[7]
    tok, width = query.shape
    heads, slots = coef.shape[:2]
    half = heads // PAIR
    vectors = step.shape[0]
    chunks = half * slots
    f32 = jnp.float32
    vmem = pl.BlockSpec(memory_space=pltpu.VMEM)
    dma = pltpu.SemaphoreType.DMA
    states = pltpu.VMEM((half, slots, HDIM, HDIM), f32)
    decays = pltpu.VMEM((half,) + coef.shape[1:], f32)
    entries = pltpu.VMEM((half, HDIM, HDIM), f32)
    products = pltpu.VMEM((half, vectors, HDIM), f32)
    return pl.pallas_call(
        functools.partial(fused_kernel, n, steps),
        out_shape=(
            jax.ShapeDtypeStruct((tok, width), f32),
            jax.ShapeDtypeStruct((8, tok), f32),
            jax.ShapeDtypeStruct((vectors, width), f32),
            jax.ShapeDtypeStruct((8, vectors), f32),
        ),
        in_specs=[vmem] * len(operands),
        out_specs=(vmem,) * 4,
        scratch_shapes=[
            states,
            states,
            states,
            decays,
            products,
            products,
            pltpu.VMEM((vectors, HDIM), f32),
            states,
            states,
            states,
            states,
            states,
            decays,
            decays,
            entries,
            pltpu.VMEM((tok, HDIM), f32),
            pltpu.VMEM((vectors, HDIM), f32),
            entries,
            entries,
            products,
            products,
            dma((chunks,)),
            dma((chunks,)),
            dma,
            dma,
            dma((half,)),
            dma((half,)),
            dma,
            dma,
            dma((chunks,)),
            dma((chunks,)),
            dma((chunks,)),
            dma((chunks,)),
            dma,
            dma,
            dma((half,)),
            dma((half,)),
            dma((half,)),
            dma((half,)),
        ],
        compiler_params=pltpu.CompilerParams(
            collective_id=0, has_side_effects=True, vmem_limit_bytes=56 * 1024 * 1024
        ),
        name="fused",
    )(*operands)


def ends_of(prompt_lengths):
    index = jnp.arange(prompt_lengths.shape[0])
    return jnp.sum(jnp.where(index[:, None] >= index[None, :], prompt_lengths[None, :], 0), axis=1)


def segment_ids(prompt_lengths, positions):
    boundary = ends_of(prompt_lengths)
    return jnp.sum((positions[:, None] >= boundary[None, :]).astype(jnp.int32), axis=1)


def local(
    n,
    query_in,
    key_in,
    value_in,
    log_decay,
    norm_gain,
    prompt_lengths,
    step_query,
    step_key,
    step_value,
    step_decay,
    row_prompt,
):
    f32 = jnp.float32
    tok = query_in.shape[0]
    heads = log_decay.shape[1]
    steps, rows = step_query.shape[:2]
    place = lax.axis_index("seq")
    first = place * tok
    pair_first = (place // PAIR) * (PAIR * tok)
    ends = ends_of(prompt_lengths)
    begins = ends - prompt_lengths
    segs = segment_ids(prompt_lengths, first + jnp.arange(tok, dtype=jnp.int32))
    slot = jnp.arange(PROMPTS, dtype=jnp.int32)

    def seg_before(token):
        return jnp.where(token > 0, segment_ids(prompt_lengths, (token - 1)[None])[0], -1)

    seg_front = seg_before(first)
    cum = jnp.cumsum(log_decay, axis=0)

    last = jnp.clip(ends - first, 1, tok) - 1
    reached = jnp.sum(
        jnp.where((jnp.arange(tok)[None, :] == last[:, None])[:, :, None], cum[None], 0.0), axis=1
    )
    taken = (segs[None, :] == slot[:, None])[:, :, None]
    keep = jnp.where(taken, jnp.exp(jnp.where(taken, reached[:, None, :] - cum[None], 0.0)), 0.0)
    carried = jnp.exp(cum) * (segs == seg_front).astype(f32)[:, None]
    spare = jnp.zeros_like(keep[:2])
    tokens = jnp.transpose(jnp.concatenate([keep, cum[None], carried[None], spare]), (2, 0, 1))
    causal = jnp.arange(tok)[:, None] >= jnp.arange(tok)[None, :]
    linked = causal & (segs[:, None] == segs[None, :])
    bias = jnp.where(linked, 0.0, -jnp.inf)
    coef = jnp.where(
        (ends <= first)[:, None], 1.0, jnp.where((begins < first)[:, None], jnp.exp(reached), 0.0)
    )
    coef = jnp.broadcast_to(coef.T[:, :, None], (heads, PROMPTS, HDIM))
    pair_last = pair_first + PAIR * tok
    marks = jnp.concatenate(
        [slot == seg_before(pair_first), slot == seg_before(pair_first + tok), ends <= pair_last]
    )
    marks = jnp.concatenate([marks, jnp.zeros((4,), bool)])
    masks = jnp.broadcast_to(marks.astype(f32)[:, None], (marks.shape[0], HDIM))

    shares = [
        [float(j < k <= i) for k in range(steps)] for i in range(steps) for j in range(i + 1)
    ]
    wholes = [[float(k <= i) for k in range(steps)] for i in range(steps)]
    step_weights = jnp.exp(
        jnp.einsum(
            "irh,wi->hrw", step_decay, jnp.array(shares + wholes, f32), precision=lax.Precision.HIGHEST
        )
    )
    row_marks = jnp.broadcast_to(
        jnp.broadcast_to(row_prompt.astype(f32)[None, :], (steps, rows)).reshape(-1, 1),
        (steps * rows, HDIM),
    )
    flat = lambda a: a.reshape(steps * rows, -1)
    mixed, mixed_sq, decoded, decoded_sq = fused(
        n,
        steps,
        query_in,
        key_in,
        value_in,
        tokens,
        bias,
        coef,
        masks,
        flat(step_query),
        flat(step_key),
        flat(step_value),
        step_weights,
        row_marks,
    )
    squares, step_squares = lax.psum(
        (mixed_sq[0], decoded_sq[0]), "head"
    )
    scale = lax.rsqrt(squares / (HEAD_COUNT * HDIM) + EPSILON)
    attn_out = (mixed * scale[:, None] * norm_gain[None, :]).astype(jnp.bfloat16)
    step_scale = lax.rsqrt(step_squares / (HEAD_COUNT * HDIM) + EPSILON)
    decode_out = (decoded * step_scale[:, None] * norm_gain[None, :]).astype(jnp.bfloat16)
    return (attn_out, decode_out.reshape(step_query.shape))


def solution(mesh):
    in_specs = (
        P("seq", "head"),
        P("seq", "head"),
        P("seq", "head"),
        P("seq", "head"),
        P("head"),
        P(),
        P(None, "seq", "head"),
        P(None, "seq", "head"),
        P(None, "seq", "head"),
        P(None, "seq", "head"),
        P("seq"),
    )
    out_specs = (P("seq", "head"), P(None, "seq", "head"))
    return jax.shard_map(
        functools.partial(local, mesh.shape["seq"]),
        mesh=mesh,
        in_specs=in_specs,
        out_specs=out_specs,
        check_vma=False,
    )
```
